256 devices in a mesh: groups: 4 (over x, y), blk: 64 (over z, core).
Axes of the slice: x: 2, y: 2, z: 32, core: 2. Of those that a mesh axis runs over, the one named last changes fastest.
The devices are a block of a 4x8x32 slice.
Arguments:
- queries: bfloat16 [8192, 8192], P('groups', 'blk'), parts along dimension 0, may hold values from -41 to 41
- prefix_kv: bfloat16 [256, 64, 8, 256], P(('groups', 'blk')), parts along dimension 0, may hold values from -6 to 6
- page_counts: int32 [16], P('groups'), parts along dimension 0, may hold values from 1 to 32, 64 in all
- request_prefix: int32 [8192, 1], P(('groups', 'blk')), parts along dimension 0, may hold values from 0 to 3
- suffix_kv: bfloat16 [8192, 64, 8, 256], P(('groups', 'blk')), parts along dimension 0, may hold values from -6 to 6
- suffix_len: int32 [8192], P(('groups', 'blk')), parts along dimension 0, may hold values from 2 to 64, as said below
Outputs:
- attended: bfloat16 [8192, 8192], P('groups', 'blk'), parts along dimension 0
The draws below stay inside these ranges and needn't reach their ends.
There are 4 independent parts, one for each index of `groups`. The reference program is written for one: setup_inputs(seed, part) draws one part's arguments, and reference() takes and returns one part's arrays. A program takes and returns all parts, laid end to end along the dimension named above; each array names one. Nothing has to cross between parts.
Inputs may be any that keep to these rules, and one draw needn't show every extreme that they name: `page_counts`: the counts sum to 64; the largest is exactly half of 64. `request_prefix`: every prefix is named by some request. `suffix_len`: the requests of one device (aligned blocks of 32) include one with 64 live positions.
All inputs are finite; a program needn't handle non-finite values.
Results may differ from the reference program's by a relative error of at most 0.013.
Values may be sent and summed in bfloat16 or wider, within the bound.
No kernel may reach another device: no remote copies, remote signals or barrier semaphores. Data moves between devices by JAX's collectives and lax.ppermute only.
A program may use at most 64 MiB of HBM per device.

```python
import math
import jax
import jax.numpy as jnp
import numpy as np
from jax import lax

NH = 64
KVH = 8
HD = 128
PAGE = 64
NPREF = 4
REQ_DEV = 32
SUF = 64
PAGES = 64
REQ = 2048


def cache_draw(key):
    base_key = jax.random.fold_in(key, 41)
    cache = jnp.clip(jax.random.normal(base_key, (REQ, SUF, KVH, 2 * HD), jnp.float32), -6.0, 6.0)
    return cache


def draw_suffix_kv(key, part):
    cache = cache_draw(key)
    return cache.astype(jnp.bfloat16)


def draw_queries(key, part):
    base_key = jax.random.fold_in(key, 61)
    rows_query = jnp.clip(2.0 * jax.random.normal(base_key, (REQ, NH * HD), jnp.float32), -12.0, 12.0)
    return rows_query.astype(jnp.bfloat16)


def draw_suffix_len(key, part):
    lengths = jax.random.randint(jax.random.fold_in(key, 31), (REQ,), 2, SUF + 1)
    chosen = jax.random.randint(jax.random.fold_in(key, 32), (REQ // REQ_DEV,), 0, REQ_DEV)
    filled = jnp.arange(REQ, dtype=jnp.int32) % REQ_DEV == jnp.repeat(chosen, REQ_DEV)
    return jnp.where(filled, SUF, lengths).astype(jnp.int32)


def level_of(stream_key, extent, cuts, low, top_value):
    def one(axis_at, shards_of):
        steps = jax.random.uniform(jax.random.fold_in(jax.random.fold_in(stream_key, 6), axis_at), (shards_of,), jnp.float32, low / len(cuts), top_value / len(cuts))
        return jnp.repeat(jnp.exp(steps), extent[axis_at] // shards_of).reshape((-1,) + (1,) * (len(extent) - axis_at - 1))

    level = one(*cuts[0])
    for cut in cuts[1:]:
        level = level * one(*cut)
    return level


def picks_of(key, rows, amount, top, lift):
    order = jax.random.permutation(jax.random.fold_in(key, 1), amount)
    boost = order
    for power in range(3):
        boost = boost * boost // amount
    boost = boost * lift // amount
    tickets = jax.random.randint(jax.random.fold_in(key, 2), (rows, amount), 0, 4096) + boost
    holders = jax.random.permutation(jax.random.fold_in(key, 3), rows)[jnp.arange(amount) % rows]
    tickets = jnp.where(jnp.arange(rows)[:, None] == holders[None, :], 1 << 14, tickets)
    merit = tickets * amount + jnp.arange(amount)
    return lax.top_k(merit.astype(jnp.int32), top)[1].astype(jnp.int32)


def length_profile(number_of, total, most, skew):
    weights = [(1 << 20) // math.isqrt(grade ** skew) + 1 for grade in range(2, number_of + 1)]
    surplus, given = total - most - (number_of - 1), [1] * (number_of - 1)
    while surplus > 0:
        candidates = [i for i in range(number_of - 1) if given[i] < most]
        pool, left = sum([weights[i] for i in candidates]), surplus
        for i in candidates:
            addition = min(most - given[i], max(1, left * weights[i] // pool), surplus)
            given[i] = given[i] + addition
            surplus = surplus - addition
    return np.array([most] + given)


def uneven_parts(own_key, number_of, total, bound, lean):
    if number_of == 2:
        one = jax.random.randint(own_key, (), max(1, total - bound), min(bound, total - 1) + 1)
        return jnp.stack([one, total - one])
    sizes = jnp.asarray(length_profile(number_of, total, bound, lean), jnp.int32)
    couples = (number_of - 1) // 2
    source_of, taker = sizes[1:1 + 2 * couples:2], sizes[2:2 + 2 * couples:2]
    slack = jnp.minimum(source_of - 1, bound - taker)
    passed = jax.random.randint(jax.random.fold_in(own_key, 1), (couples,), 0, 1 << 20) % (slack + 1)
    sizes = sizes.at[1:1 + 2 * couples:2].set(source_of - passed).at[2:2 + 2 * couples:2].set(taker + passed)
    return sizes[jax.random.permutation(jax.random.fold_in(own_key, 2), number_of)]


def scatter_about(key, extent, scale, bound, shards=(), kind=jnp.bfloat16):
    values = jax.random.normal(key, extent, jnp.float32) * scale
    if len(shards) > 0:
        values = level_of(key, extent, shards, -0.22, 0.18) * values
    return jnp.clip(values, min=-bound, max=bound).astype(kind)


def setup_inputs(seed: int = 0, part: int = 0) -> dict:
    splits = jax.random.split(jax.random.key(seed), 7)
    part_splits = jax.random.split(jax.random.fold_in(splits[6], part), 7)
    return {
        "queries": draw_queries(jax.random.fold_in(jax.random.fold_in(splits[6], part), 71), part),
        "prefix_kv": scatter_about(part_splits[1], (PAGES, PAGE, KVH, 2 * HD), 1.0, 6.0, ((0, 64),)),
        "page_counts": uneven_parts(part_splits[2], NPREF, PAGES, PAGES // 2, 2).astype(jnp.int32),
        "request_prefix": picks_of(part_splits[3], REQ, NPREF, 1, 4096),
        "suffix_kv": draw_suffix_kv(jax.random.fold_in(jax.random.fold_in(splits[6], part), 71), part),
        "suffix_len": draw_suffix_len(jax.random.fold_in(jax.random.fold_in(splits[6], part), 71), part),
    }


neg_large = -1.0e30


def reference(queries, prefix_kv, page_counts, request_prefix, suffix_kv, suffix_len):
    group_size = NH // KVH
    score_scale = HD ** -0.5
    page_ends = jnp.cumsum(page_counts)
    page_index = jnp.arange(PAGES, dtype=jnp.int32)
    page_owner = jnp.sum((page_index[:, None] >= page_ends[None, :]).astype(jnp.int32), axis=1)
    token_owner = jnp.repeat(page_owner, PAGE)
    pooled = prefix_kv.reshape(PAGES * PAGE, KVH, 2 * HD).astype(jnp.float32)
    pool_keys = pooled[:, :, :HD]
    pool_values = pooled[:, :, HD:]
    block_count = REQ // REQ_DEV

    def one_block(pieces):
        rows_query, rows_owner, rows_cache, rows_length = pieces
        query_full = rows_query.astype(jnp.float32).reshape(REQ_DEV, KVH, group_size, HD)
        cache_full = rows_cache.astype(jnp.float32)
        prefix_scores = jnp.einsum("rkgd,tkd->rkgt", query_full, pool_keys) * score_scale
        suffix_scores = jnp.einsum("rkgd,rtkd->rkgt", query_full, cache_full[..., :HD]) * score_scale
        prefix_live = (rows_owner[:, None] == token_owner[None, :])[:, None, None, :]
        suffix_live = (jnp.arange(SUF, dtype=jnp.int32)[None, :] < rows_length[:, None])[:, None, None, :]
        prefix_scores = jnp.where(prefix_live, prefix_scores, neg_large)
        suffix_scores = jnp.where(suffix_live, suffix_scores, neg_large)
        top_score = jnp.maximum(jnp.max(prefix_scores, axis=-1), jnp.max(suffix_scores, axis=-1))
        prefix_weight = jnp.where(prefix_live, jnp.exp(prefix_scores - top_score[..., None]), 0.0)
        suffix_weight = jnp.where(suffix_live, jnp.exp(suffix_scores - top_score[..., None]), 0.0)
        weight_sum = jnp.sum(prefix_weight, axis=-1) + jnp.sum(suffix_weight, axis=-1)
        prefix_round = lax.optimization_barrier(prefix_weight.astype(jnp.bfloat16)).astype(jnp.float32)
        suffix_round = lax.optimization_barrier(suffix_weight.astype(jnp.bfloat16)).astype(jnp.float32)
        mixed_sum = jnp.einsum("rkgt,tkd->rkgd", prefix_round, pool_values)
        mixed_sum = mixed_sum + jnp.einsum("rkgt,rtkd->rkgd", suffix_round, cache_full[..., HD:])
        result = (mixed_sum / weight_sum[..., None]).astype(jnp.bfloat16)
        return result.reshape(REQ_DEV, NH * HD)

    outputs = lax.map(one_block, (
        queries.reshape(block_count, REQ_DEV, NH * HD),
        request_prefix.reshape(block_count, REQ_DEV),
        suffix_kv.reshape(block_count, REQ_DEV, SUF, KVH, 2 * HD),
        suffix_len.reshape(block_count, REQ_DEV)))
    return outputs.reshape(REQ, NH * HD)
```

```python
import functools

import jax
import jax.numpy as jnp
from jax import lax
from jax.experimental import pallas as pl
from jax.experimental.pallas import tpu as pltpu
from jax.sharding import Mesh
from jax.sharding import PartitionSpec as P

SEGS = 8
CORES = 2
BLK = ("seg", "chip", "core")
GROUPS_BLK = ("groups", "seg", "chip", "core")


LOG2E = 1.4426950408889634
LN2 = 0.6931471805599453
NEG = -1e30

REQ_STEP = 4
TOK_BLOCK = 512
ROW_BLOCK = 512

NT = (((1,), (1,)), ((), ()))


def f32(x):
    return x.astype(jnp.float32)


def bf16(x):
    return x.astype(jnp.bfloat16)


def suffix_kernel(len_ref, got_ref, owner_ref, kv_ref, out_ref, q_scr, o_scr, lse_scr, bias_scr, *, req_dev, heads, kv_heads):
    step = pl.program_id(0)
    hd = q_scr.shape[1]
    cols = kv_ref.shape[1]
    stride = out_ref.shape[0] // heads
    scale = hd**-0.5 * LOG2E
    lane = lax.broadcasted_iota(jnp.int32, (heads, hd), 1)

    @pl.when(step == 0)
    def _():
        for h in range(heads):
            q_scr[pl.ds(h, req_dev, stride=heads), :] = f32(got_ref[h, 0:req_dev, :])
        row = lax.broadcasted_iota(jnp.int32, (heads, cols), 0)
        col = lax.broadcasted_iota(jnp.int32, (heads, cols), 1)
        same = (col % kv_heads) == (row // (heads // kv_heads))
        bias_scr[...] = jnp.where(same, 0.0, NEG)
        lse_scr[...] = jnp.zeros_like(lse_scr)

    col = lax.broadcasted_iota(jnp.int32, (1, cols), 1)
    lse = lse_scr[...]
    for i in range(REQ_STEP):
        r = step * REQ_STEP + i
        q = bf16(q_scr[pl.ds(pl.multiple_of(r * heads, heads), heads), :])
        s = lax.dot_general(q, kv_ref[i, :, 0:hd], NT, preferred_element_type=jnp.float32)
        past = jnp.where(col < len_ref[r] * kv_heads, 0.0, NEG)
        s = s * scale + (bias_scr[...] + past)
        top = jnp.max(s, axis=1, keepdims=True)
        w = jnp.exp2(s - top)
        total = jnp.sum(w, axis=1, keepdims=True)
        o = jnp.dot(bf16(w), kv_ref[i, :, hd:], preferred_element_type=jnp.float32) / total
        o_scr[pl.ds(r, heads, stride=stride), :] = o
        value = top * LN2 + jnp.log(total)
        lse = jnp.where((lane % req_dev) == r, value, lse)
    lse_scr[...] = lse

    @pl.when(step == pl.num_programs(0) - 1)
    def _():
        hi = f32(bf16(lse))
        rest = lse - hi
        mid = f32(bf16(rest))
        low = rest - mid
        extra = jnp.where(lane < req_dev, hi, jnp.where(lane < 2 * req_dev, mid, low))
        extra = jnp.where(lane < 3 * req_dev, extra, owner_ref[...])
        o_scr[pl.ds(req_dev, heads, stride=stride), :] = extra
        o_scr[pl.ds(req_dev + 1, heads, stride=stride), :] = jnp.zeros((heads, hd), jnp.float32)
        n = out_ref.shape[0]
        c = n // 17 if n % 17 == 0 else n

        @pl.loop(0, n // c)
        def _(k):
            at = pl.ds(pl.multiple_of(k * c, 16), c)
            out_ref[at, :] = bf16(o_scr[at, :])


def suffix_attention(got, owner_row, suffix_kv, suffix_len):
    req_dev, suf, kv_heads, width = suffix_kv.shape
    hd = width // 2
    heads = got.shape[0]
    cache = suffix_kv.reshape(req_dev, suf * kv_heads, width)
    rows = heads * (req_dev + 2)
    kernel = functools.partial(suffix_kernel, req_dev=req_dev, heads=heads, kv_heads=kv_heads)
    return pl.pallas_call(
        kernel,
        name="suffix",
        out_shape=jax.ShapeDtypeStruct((rows, hd), jnp.bfloat16),
        grid_spec=pltpu.PrefetchScalarGridSpec(
            num_scalar_prefetch=1,
            grid=(req_dev // REQ_STEP,),
            in_specs=[
                pl.BlockSpec(got.shape, lambda i, n: (0, 0, 0)),
                pl.BlockSpec(owner_row.shape, lambda i, n: (0, 0)),
                pl.BlockSpec((REQ_STEP, suf * kv_heads, width), lambda i, n: (i, 0, 0)),
            ],
            out_specs=pl.BlockSpec((rows, hd), lambda i, n: (0, 0)),
            scratch_shapes=[
                pltpu.VMEM((req_dev * heads, hd), jnp.float32),
                pltpu.VMEM((rows, hd), jnp.float32),
                pltpu.VMEM((heads, hd), jnp.float32),
                pltpu.VMEM((heads, suf * kv_heads), jnp.float32),
            ],
        ),
        cost_estimate=pl.CostEstimate(
            flops=4 * req_dev * heads * suf * kv_heads * hd,
            bytes_accessed=2 * suffix_kv.size,
            transcendentals=req_dev * heads * suf * kv_heads,
        ),
    )(suffix_len, got, owner_row, cache)


def prefix_kernel(count_ref, q_ref, *refs, req_dev, n_chunks):
    chunks = refs[:n_chunks]
    o_ref, lse_ref, k_scr, v_scr, top_scr, sum_scr, acc_scr = refs[n_chunks:]
    n_prefix = o_ref.shape[0]
    n_rows, hd = q_ref.shape
    pages, both = chunks[0].shape[:2]
    tok = both // 2
    page = tok * n_chunks
    scale = hd**-0.5 * LOG2E
    tail = k_scr.shape[0] - pages * page

    @pl.loop(0, pages)
    def _(p):
        for c in range(0, n_chunks, 2):
            a, b = f32(chunks[c][p]), f32(chunks[c + 1][p])
            at = pl.ds(pl.multiple_of(p * page + c * tok, 2 * tok), 2 * tok)
            k_scr[at, :] = bf16(jnp.concatenate([a[:tok], b[:tok]], axis=0))
            v_scr[at, :] = bf16(jnp.concatenate([a[tok:], b[tok:]], axis=0))

    k_scr[pl.ds(pages * page, tail), :] = jnp.zeros((tail, hd), jnp.bfloat16)
    v_scr[pl.ds(pages * page, tail), :] = jnp.zeros((tail, hd), jnp.bfloat16)

    col = lax.broadcasted_iota(jnp.int32, (1, TOK_BLOCK), 1)
    lane = lax.broadcasted_iota(jnp.int32, (req_dev, lse_ref.shape[2]), 1)
    for p in range(n_prefix):
        lse_ref[p] = jnp.zeros(lse_ref.shape[1:], jnp.float32)
    first = 0
    for p in range(n_prefix):
        start = first * page
        live = count_ref[p] * page

        @pl.loop(0, n_rows // ROW_BLOCK)
        def _(rb):
            rows = pl.ds(pl.multiple_of(rb * ROW_BLOCK, ROW_BLOCK), ROW_BLOCK)
            top_scr[...] = jnp.full_like(top_scr, NEG)
            sum_scr[...] = jnp.zeros_like(sum_scr)
            acc_scr[...] = jnp.zeros_like(acc_scr)

            @pl.loop(0, (live + TOK_BLOCK - 1) // TOK_BLOCK)
            def _(b):
                at = pl.ds(pl.multiple_of(start + b * TOK_BLOCK, page), TOK_BLOCK)
                s = lax.dot_general(q_ref[rows, :], k_scr[at, :], NT, preferred_element_type=jnp.float32)
                past = jnp.where(col < live - b * TOK_BLOCK, 0.0, NEG)
                s = s * scale + past
                old = top_scr[...]
                new = jnp.maximum(old, jnp.max(s, axis=1, keepdims=True))
                alpha = jnp.exp2(old - new)
                w = jnp.exp2(s - new[:, 0:1])
                part = w[:, 0:hd]
                for k in range(hd, TOK_BLOCK, hd):
                    part = part + w[:, k : k + hd]
                top_scr[...] = new
                sum_scr[...] = sum_scr[...] * alpha + part
                acc_scr[...] = acc_scr[...] * alpha + jnp.dot(
                    bf16(w), v_scr[at, :], preferred_element_type=jnp.float32
                )

            total = jnp.sum(sum_scr[...], axis=1, keepdims=True)
            o_ref[p, rows, :] = bf16(acc_scr[...] / total)
            value = top_scr[...][:, 0:1] * LN2 + jnp.log(total)
            lse = lse_ref[p]
            for k in range(ROW_BLOCK // req_dev):
                piece = value[k * req_dev : (k + 1) * req_dev, :]
                lse = jnp.where(lane == rb * (ROW_BLOCK // req_dev) + k, piece, lse)
            lse_ref[p] = lse

        first = first + count_ref[p]


def prefix_attention(queries, chunks, page_counts, req_dev):
    n_rows, hd = queries.shape
    n_prefix = page_counts.shape[0]
    pages, both, _ = chunks[0].shape
    tokens = pages * (both // 2) * len(chunks)
    vmem = pl.BlockSpec(memory_space=pltpu.VMEM)
    kernel = functools.partial(prefix_kernel, req_dev=req_dev, n_chunks=len(chunks))
    return pl.pallas_call(
        kernel,
        name="prefix",
        out_shape=(
            jax.ShapeDtypeStruct((n_prefix, n_rows, hd), jnp.bfloat16),
            jax.ShapeDtypeStruct((n_prefix, req_dev, hd), jnp.float32),
        ),
        in_specs=[pl.BlockSpec(memory_space=pltpu.SMEM)] + [vmem] * (1 + len(chunks)),
        out_specs=(vmem, vmem),
        scratch_shapes=[
            pltpu.VMEM((tokens + TOK_BLOCK, hd), jnp.bfloat16),
            pltpu.VMEM((tokens + TOK_BLOCK, hd), jnp.bfloat16),
            pltpu.VMEM((ROW_BLOCK, hd), jnp.float32),
            pltpu.VMEM((ROW_BLOCK, hd), jnp.float32),
            pltpu.VMEM((ROW_BLOCK, hd), jnp.float32),
        ],
        cost_estimate=pl.CostEstimate(
            flops=4 * n_rows * tokens * hd, bytes_accessed=4 * n_rows * hd, transcendentals=n_rows * tokens
        ),
    )(page_counts, queries, *chunks)


def combine_kernel(got_ref, o_ref, lse_ref, out_ref, scr, *, req_dev):
    n, hd = scr.shape
    stride = req_dev + 2
    blocks = n // stride
    n_prefix = o_ref.shape[0]
    c = n // 17 if n % 17 == 0 else n

    @pl.loop(0, n // c)
    def _(k):
        at = pl.ds(pl.multiple_of(k * c, 16), c)
        scr[at, :] = f32(got_ref[at, :])

    extra = scr[pl.ds(req_dev, blocks, stride=stride), :].T
    tall = [extra[k * req_dev : (k + 1) * req_dev, :] for k in range(4)]
    suffix_lse = tall[0] + tall[1] + tall[2]
    owner = tall[3]
    prefix_lse = lse_ref[0][:, 0:blocks]
    for p in range(1, n_prefix):
        prefix_lse = jnp.where(owner == p, lse_ref[p][:, 0:blocks], prefix_lse)
    top = jnp.maximum(suffix_lse, prefix_lse)
    ws = jnp.exp(suffix_lse - top)
    wp = jnp.exp(prefix_lse - top)
    inverse = 1.0 / (ws + wp)
    ws, wp = ws * inverse, wp * inverse
    for j in range(blocks):
        rows = slice(j * req_dev, (j + 1) * req_dev)
        own = jnp.broadcast_to(owner[:, j : j + 1], (req_dev, hd))
        part = f32(o_ref[0, rows, :])
        for p in range(1, n_prefix):
            part = jnp.where(own == p, f32(o_ref[p, rows, :]), part)
        mine = scr[pl.ds(j * stride, req_dev), :]
        out_ref[rows, :] = bf16(mine * ws[:, j : j + 1] + part * wp[:, j : j + 1])


def combine(got, prefix_o, prefix_lse, req_dev):
    n_rows, hd = prefix_o.shape[1:]
    vmem = pl.BlockSpec(memory_space=pltpu.VMEM)
    return pl.pallas_call(
        functools.partial(combine_kernel, req_dev=req_dev),
        name="combine",
        out_shape=jax.ShapeDtypeStruct((n_rows, hd), jnp.bfloat16),
        in_specs=[vmem] * 3,
        out_specs=vmem,
        scratch_shapes=[pltpu.VMEM(got.shape, jnp.float32)],
        cost_estimate=pl.CostEstimate(flops=10 * n_rows * hd, bytes_accessed=12 * n_rows * hd, transcendentals=0),
    )(got, prefix_o, prefix_lse)


def exchange(x):
    return lax.all_to_all(x, BLK, split_axis=0, concat_axis=0, tiled=True)


def body(queries, prefix_kv, page_counts, request_prefix, suffix_kv, suffix_len):
    blocks = lax.axis_size(BLK)
    req_dev = suffix_kv.shape[0]
    kv_heads = suffix_kv.shape[2]
    hd = suffix_kv.shape[3] // 2
    page = prefix_kv.shape[1]
    share = blocks // kv_heads
    tok = page // share

    mine = prefix_kv[0].reshape(share, tok, kv_heads, 2, hd).transpose(2, 0, 3, 1, 4)
    mine = mine.reshape(blocks, 2 * tok, hd)
    got = exchange(jnp.concatenate([queries.reshape(blocks, req_dev, hd), mine], axis=1))

    own = got[:, req_dev:, :]
    chips = lax.axis_size("chip")
    chunks = [own] + [lax.ppermute(own, "chip", [(i, (i + k) % chips) for i in range(chips)]) for k in range(1, chips)]
    swap = [(i, CORES - 1 - i) for i in range(CORES)]
    chunks = chunks + [lax.ppermute(c, "core", swap) for c in chunks]

    owner = request_prefix[:, 0].astype(jnp.float32)[None, :]
    owner_row = jnp.pad(owner, ((0, 0), (hd - req_dev, 0)))
    sent = suffix_attention(got, owner_row, suffix_kv, suffix_len)
    back = exchange(sent.reshape(blocks, (req_dev + 2) // 2, 2, hd)).reshape(sent.shape)

    prefix_o, prefix_lse = prefix_attention(queries, chunks, page_counts, req_dev)
    return combine(back, prefix_o, prefix_lse, req_dev)


def solution(mesh):
    chips = mesh.shape["blk"] // (SEGS * CORES)
    split = Mesh(
        mesh.devices.reshape(mesh.shape["groups"], SEGS, chips, CORES), ("groups", "seg", "chip", "core")
    )
    in_specs = (
        P("groups", BLK),
        P(GROUPS_BLK, None, None, None),
        P("groups"),
        P(GROUPS_BLK, None),
        P(GROUPS_BLK, None, None, None),
        P(GROUPS_BLK),
    )
    return jax.shard_map(body, mesh=split, in_specs=in_specs, out_specs=P("groups", BLK), check_vma=False)
```

```python
import functools

import jax
import jax.numpy as jnp
from jax import lax
from jax.experimental import pallas as pl
from jax.experimental.pallas import tpu as pltpu
from jax.sharding import Mesh
from jax.sharding import PartitionSpec as P

SEGS = 8
CORES = 2
BLK = ("seg", "chip", "core")
GROUPS_BLK = ("groups", "seg", "chip", "core")


LOG2E = 1.4426950408889634
LN2 = 0.6931471805599453
NEG = -1e30

REQ_STEP = 8
TOK_BLOCK = 512
ROW_BLOCK = 512

NT = (((1,), (1,)), ((), ()))


def f32(x):
    return x.astype(jnp.float32)


def bf16(x):
    return x.astype(jnp.bfloat16)


def suffix_kernel(
    len_ref, got_ref, owner_ref, cache_ref, out_ref, kv_ref, sems, q_scr, o_scr, s_scr, w_scr, t_scr, bias_scr, *, req_dev, heads, kv_heads
):
    def fetch(step):
        at = pl.ds(step * REQ_STEP, REQ_STEP)
        return pltpu.make_async_copy(cache_ref.at[at], kv_ref.at[at], sems.at[step])

    for step in range(req_dev // REQ_STEP):
        fetch(step).start()
    hd = q_scr.shape[1]
    cols = kv_ref.shape[1]
    stride = out_ref.shape[0] // heads
    scale = hd**-0.5 * LOG2E
    lane = lax.broadcasted_iota(jnp.int32, (heads, hd), 1)

    for h in range(heads):
        q_scr[pl.ds(h, req_dev, stride=heads), :] = f32(got_ref[h, 0:req_dev, :])
    row = lax.broadcasted_iota(jnp.int32, (heads, cols), 0)
    col = lax.broadcasted_iota(jnp.int32, (heads, cols), 1)
    same = (col % kv_heads) == (row // (heads // kv_heads))
    bias_scr[...] = jnp.where(same, 0.0, NEG)
    col = lax.broadcasted_iota(jnp.int32, (1, cols), 1)

    steps = req_dev // REQ_STEP
    lse = jnp.zeros((heads, hd), jnp.float32)

    def scores(t):
        for i in range(REQ_STEP):
            r = t * REQ_STEP + i
            q = bf16(q_scr[r * heads : (r + 1) * heads, :])
            s_scr[t % 2, i] = lax.dot_general(q, kv_ref[r, :, 0:hd], NT, preferred_element_type=jnp.float32)

    def weights(t, lse):
        for i in range(REQ_STEP):
            r = t * REQ_STEP + i
            past = jnp.where(col < len_ref[r] * kv_heads, 0.0, NEG)
            s = s_scr[t % 2, i] * scale + (bias_scr[...] + past)
            top = jnp.max(s, axis=1, keepdims=True)
            w = jnp.exp2(s - top)
            total = jnp.sum(w, axis=1, keepdims=True)
            w_scr[t % 2, i] = bf16(w)
            t_scr[t % 2, i] = jnp.broadcast_to(total, (heads, hd))
            lse = jnp.where((lane % req_dev) == r, top * LN2 + jnp.log(total), lse)
        return lse

    def mix(t):
        for i in range(REQ_STEP):
            r = t * REQ_STEP + i
            o = jnp.dot(w_scr[t % 2, i], kv_ref[r, :, hd:], preferred_element_type=jnp.float32)
            o_scr[pl.ds(r, heads, stride=stride), :] = o / t_scr[t % 2, i]

    for t in range(steps + 2):
        if t < steps:
            fetch(t).wait()
            scores(t)
        if 0 <= t - 1 < steps:
            lse = weights(t - 1, lse)
        if t >= 2:
            mix(t - 2)

    hi = f32(bf16(lse))
    rest = lse - hi
    mid = f32(bf16(rest))
    low = rest - mid
    extra = jnp.where(lane < req_dev, hi, jnp.where(lane < 2 * req_dev, mid, low))
    extra = jnp.where(lane < 3 * req_dev, extra, owner_ref[...])
    o_scr[pl.ds(req_dev, heads, stride=stride), :] = extra
    o_scr[pl.ds(req_dev + 1, heads, stride=stride), :] = jnp.zeros((heads, hd), jnp.float32)
    n = out_ref.shape[0]
    c = n // 17 if n % 17 == 0 else n

    @pl.loop(0, n // c)
    def _(k):
        at = pl.ds(pl.multiple_of(k * c, 16), c)
        out_ref[at, :] = bf16(o_scr[at, :])


def suffix_attention(got, owner_row, cache, suffix_len, kv_heads):
    req_dev, cols, width = cache.shape
    hd = width // 2
    heads = got.shape[0]
    rows = heads * (req_dev + 2)
    kernel = functools.partial(suffix_kernel, req_dev=req_dev, heads=heads, kv_heads=kv_heads)
    vmem = pl.BlockSpec(memory_space=pltpu.VMEM)
    return pl.pallas_call(
        kernel,
        name="suffix",
        out_shape=jax.ShapeDtypeStruct((rows, hd), jnp.bfloat16),
        in_specs=[pl.BlockSpec(memory_space=pltpu.SMEM), vmem, vmem, pl.BlockSpec(memory_space=pltpu.HBM)],
        out_specs=vmem,
        scratch_shapes=[
            pltpu.VMEM(cache.shape, cache.dtype),
            pltpu.SemaphoreType.DMA((req_dev // REQ_STEP,)),
            pltpu.VMEM((req_dev * heads, hd), jnp.float32),
            pltpu.VMEM((rows, hd), jnp.float32),
            pltpu.VMEM((2, REQ_STEP, heads, cols), jnp.float32),
            pltpu.VMEM((2, REQ_STEP, heads, cols), jnp.bfloat16),
            pltpu.VMEM((2, REQ_STEP, heads, hd), jnp.float32),
            pltpu.VMEM((heads, cols), jnp.float32),
        ],
        compiler_params=pltpu.CompilerParams(vmem_limit_bytes=57 << 20),
        cost_estimate=pl.CostEstimate(
            flops=4 * req_dev * heads * cols * hd,
            bytes_accessed=2 * cache.size,
            transcendentals=req_dev * heads * cols,
        ),
    )(suffix_len, got, owner_row, cache)


def prefix_kernel(count_ref, q_ref, *refs, req_dev, n_chunks):
    chunks = refs[:n_chunks]
    o_ref, lse_ref, k_scr, v_scr, top_scr, sum_scr, acc_scr = refs[n_chunks:]
    n_prefix = o_ref.shape[0]
    n_rows, hd = q_ref.shape
    pages, both = chunks[0].shape[:2]
    tok = both // 2
    page = tok * n_chunks
    scale = hd**-0.5 * LOG2E
    tail = k_scr.shape[0] - pages * page

    @pl.loop(0, pages)
    def _(p):
        for c in range(0, n_chunks, 2):
            a, b = f32(chunks[c][p]), f32(chunks[c + 1][p])
            at = pl.ds(pl.multiple_of(p * page + c * tok, 2 * tok), 2 * tok)
            k_scr[at, :] = bf16(jnp.concatenate([a[:tok], b[:tok]], axis=0))
            v_scr[at, :] = bf16(jnp.concatenate([a[tok:], b[tok:]], axis=0))

    k_scr[pl.ds(pages * page, tail), :] = jnp.zeros((tail, hd), jnp.bfloat16)
    v_scr[pl.ds(pages * page, tail), :] = jnp.zeros((tail, hd), jnp.bfloat16)

    col = lax.broadcasted_iota(jnp.int32, (1, TOK_BLOCK), 1)
    lane = lax.broadcasted_iota(jnp.int32, (req_dev, lse_ref.shape[2]), 1)
    for p in range(n_prefix):
        lse_ref[p] = jnp.zeros(lse_ref.shape[1:], jnp.float32)
    first = 0
    for p in range(n_prefix):
        start = first * page
        live = count_ref[p] * page

        @pl.loop(0, n_rows // ROW_BLOCK)
        def _(rb):
            rows = pl.ds(pl.multiple_of(rb * ROW_BLOCK, ROW_BLOCK), ROW_BLOCK)
            top_scr[...] = jnp.full_like(top_scr, NEG)
            sum_scr[...] = jnp.zeros_like(sum_scr)
            acc_scr[...] = jnp.zeros_like(acc_scr)

            @pl.loop(0, (live + TOK_BLOCK - 1) // TOK_BLOCK)
            def _(b):
                at = pl.ds(pl.multiple_of(start + b * TOK_BLOCK, page), TOK_BLOCK)
                s = lax.dot_general(q_ref[rows, :], k_scr[at, :], NT, preferred_element_type=jnp.float32)
                past = jnp.where(col < live - b * TOK_BLOCK, 0.0, NEG)
                s = s * scale + past
                old = top_scr[...]
                new = jnp.maximum(old, jnp.max(s, axis=1, keepdims=True))
                alpha = jnp.exp2(old - new)
                w = jnp.exp2(s - new[:, 0:1])
                part = w[:, 0:hd]
                for k in range(hd, TOK_BLOCK, hd):
                    part = part + w[:, k : k + hd]
                top_scr[...] = new
                sum_scr[...] = sum_scr[...] * alpha + part
                acc_scr[...] = acc_scr[...] * alpha + jnp.dot(
                    bf16(w), v_scr[at, :], preferred_element_type=jnp.float32
                )

            total = jnp.sum(sum_scr[...], axis=1, keepdims=True)
            o_ref[p, rows, :] = bf16(acc_scr[...] / total)
            value = top_scr[...][:, 0:1] * LN2 + jnp.log(total)
            lse = lse_ref[p]
            for k in range(ROW_BLOCK // req_dev):
                piece = value[k * req_dev : (k + 1) * req_dev, :]
                lse = jnp.where(lane == rb * (ROW_BLOCK // req_dev) + k, piece, lse)
            lse_ref[p] = lse

        first = first + count_ref[p]


def prefix_attention(queries, chunks, page_counts, req_dev):
    n_rows, hd = queries.shape
    n_prefix = page_counts.shape[0]
    pages, both, _ = chunks[0].shape
    tokens = pages * (both // 2) * len(chunks)
    vmem = pl.BlockSpec(memory_space=pltpu.VMEM)
    kernel = functools.partial(prefix_kernel, req_dev=req_dev, n_chunks=len(chunks))
    return pl.pallas_call(
        kernel,
        name="prefix",
        out_shape=(
            jax.ShapeDtypeStruct((n_prefix, n_rows, hd), jnp.bfloat16),
            jax.ShapeDtypeStruct((n_prefix, req_dev, hd), jnp.float32),
        ),
        in_specs=[pl.BlockSpec(memory_space=pltpu.SMEM)] + [vmem] * (1 + len(chunks)),
        out_specs=(vmem, vmem),
        scratch_shapes=[
            pltpu.VMEM((tokens + TOK_BLOCK, hd), jnp.bfloat16),
            pltpu.VMEM((tokens + TOK_BLOCK, hd), jnp.bfloat16),
            pltpu.VMEM((ROW_BLOCK, hd), jnp.float32),
            pltpu.VMEM((ROW_BLOCK, hd), jnp.float32),
            pltpu.VMEM((ROW_BLOCK, hd), jnp.float32),
        ],
        compiler_params=pltpu.CompilerParams(vmem_limit_bytes=24 << 20),
        cost_estimate=pl.CostEstimate(
            flops=4 * n_rows * tokens * hd, bytes_accessed=4 * n_rows * hd, transcendentals=n_rows * tokens
        ),
    )(page_counts, queries, *chunks)


def combine_kernel(got_ref, o_ref, lse_ref, out_ref, scr, *, req_dev):
    n, hd = scr.shape
    stride = req_dev + 2
    blocks = n // stride
    n_prefix = o_ref.shape[0]
    c = n // 17 if n % 17 == 0 else n

    @pl.loop(0, n // c)
    def _(k):
        at = pl.ds(pl.multiple_of(k * c, 16), c)
        scr[at, :] = f32(got_ref[at, :])

    extra = scr[pl.ds(req_dev, blocks, stride=stride), :].T
    tall = [extra[k * req_dev : (k + 1) * req_dev, :] for k in range(4)]
    suffix_lse = tall[0] + tall[1] + tall[2]
    owner = tall[3]
    prefix_lse = lse_ref[0][:, 0:blocks]
    for p in range(1, n_prefix):
        prefix_lse = jnp.where(owner == p, lse_ref[p][:, 0:blocks], prefix_lse)
    top = jnp.maximum(suffix_lse, prefix_lse)
    ws = jnp.exp(suffix_lse - top)
    wp = jnp.exp(prefix_lse - top)
    inverse = 1.0 / (ws + wp)
    ws, wp = ws * inverse, wp * inverse
    for j in range(blocks):
        rows = slice(j * req_dev, (j + 1) * req_dev)
        own = jnp.broadcast_to(owner[:, j : j + 1], (req_dev, hd))
        part = f32(o_ref[0, rows, :])
        for p in range(1, n_prefix):
            part = jnp.where(own == p, f32(o_ref[p, rows, :]), part)
        mine = scr[pl.ds(j * stride, req_dev), :]
        out_ref[rows, :] = bf16(mine * ws[:, j : j + 1] + part * wp[:, j : j + 1])


def combine(got, prefix_o, prefix_lse, req_dev):
    n_rows, hd = prefix_o.shape[1:]
    vmem = pl.BlockSpec(memory_space=pltpu.VMEM)
    return pl.pallas_call(
        functools.partial(combine_kernel, req_dev=req_dev),
        name="combine",
        out_shape=jax.ShapeDtypeStruct((n_rows, hd), jnp.bfloat16),
        in_specs=[vmem] * 3,
        out_specs=vmem,
        scratch_shapes=[pltpu.VMEM(got.shape, jnp.float32)],
        compiler_params=pltpu.CompilerParams(vmem_limit_bytes=16 << 20),
        cost_estimate=pl.CostEstimate(flops=10 * n_rows * hd, bytes_accessed=12 * n_rows * hd, transcendentals=0),
    )(got, prefix_o, prefix_lse)


def exchange(x):
    return lax.all_to_all(x, BLK, split_axis=0, concat_axis=0, tiled=True)


def body(queries, prefix_kv, page_counts, request_prefix, suffix_kv, suffix_len):
    blocks = lax.axis_size(BLK)
    req_dev = suffix_kv.shape[0]
    kv_heads = suffix_kv.shape[2]
    hd = suffix_kv.shape[3] // 2
    page = prefix_kv.shape[1]
    share = blocks // kv_heads
    tok = page // share

    mine = prefix_kv[0].reshape(share, tok, kv_heads, 2, hd).transpose(2, 0, 3, 1, 4)
    mine = mine.reshape(blocks, 2 * tok, hd)
    got = exchange(jnp.concatenate([queries.reshape(blocks, req_dev, hd), mine], axis=1))

    own = got[:, req_dev:, :]
    chips = lax.axis_size("chip")
    swap = [(i, CORES - 1 - i) for i in range(CORES)]
    chunks = [own]
    owner = request_prefix[:, 0].astype(jnp.float32)[None, :]
    owner_row = jnp.pad(owner, ((0, 0), (hd - req_dev, 0)))
    for k in range(1, chips):
        chunks.append(lax.ppermute(own, "chip", [(i, (i + k) % chips) for i in range(chips)]))
    chunks = chunks + [lax.ppermute(c, "core", swap) for c in chunks]
    sent = suffix_attention(got, owner_row, suffix_kv.reshape(req_dev, -1, 2 * hd), suffix_len, kv_heads)
    back = exchange(sent.reshape(blocks, (req_dev + 2) // 2, 2, hd)).reshape(sent.shape)
    prefix_o, prefix_lse = prefix_attention(queries, chunks, page_counts, req_dev)
    return combine(back, prefix_o, prefix_lse, req_dev)


def solution(mesh):
    chips = mesh.shape["blk"] // (SEGS * CORES)
    split = Mesh(
        mesh.devices.reshape(mesh.shape["groups"], SEGS, chips, CORES), ("groups", "seg", "chip", "core")
    )
    in_specs = (
        P("groups", BLK),
        P(GROUPS_BLK, None, None, None),
        P("groups"),
        P(GROUPS_BLK, None),
        P(GROUPS_BLK, None, None, None),
        P(GROUPS_BLK),
    )
    return jax.shard_map(body, mesh=split, in_specs=in_specs, out_specs=P("groups", BLK), check_vma=False)
```

```python
import functools

import jax
import jax.numpy as jnp
from jax import lax
from jax.experimental import pallas as pl
from jax.experimental.pallas import tpu as pltpu
from jax.sharding import Mesh
from jax.sharding import PartitionSpec as P

SEGS = 8
CORES = 2
BLK = ("seg", "chip", "core")
GROUPS_BLK = ("groups", "seg", "chip", "core")


LOG2E = 1.4426950408889634
LN2 = 0.6931471805599453
NEG = -1e30

REQ_STEP = 8
EARLY_BLOCK = 256
LATE_BLOCK = 512
ROW_BLOCK = 2048

NT = (((1,), (1,)), ((), ()))


def f32(x):
    return x.astype(jnp.float32)


def bf16(x):
    return x.astype(jnp.bfloat16)


def suffix_kernel(
    len_ref, got_ref, owner_ref, cache_ref, out_ref, kv_ref, sems, q_scr, o_scr, s_scr, w_scr, t_scr, bias_scr, *, req_dev, heads, kv_heads
):
    def fetch(step):
        at = pl.ds(step * REQ_STEP, REQ_STEP)
        return pltpu.make_async_copy(cache_ref.at[at], kv_ref.at[at], sems.at[step])

    for step in range(req_dev // REQ_STEP):
        fetch(step).start()
    hd = q_scr.shape[1]
    cols = kv_ref.shape[1]
    stride = out_ref.shape[0] // heads
    scale = hd**-0.5 * LOG2E
    lane = lax.broadcasted_iota(jnp.int32, (heads, hd), 1)

    for h in range(heads):
        q_scr[pl.ds(h, req_dev, stride=heads), :] = f32(got_ref[h, 0:req_dev, :])
    row = lax.broadcasted_iota(jnp.int32, (heads, cols), 0)
    col = lax.broadcasted_iota(jnp.int32, (heads, cols), 1)
    same = (col % kv_heads) == (row // (heads // kv_heads))
    bias_scr[...] = jnp.where(same, 0.0, NEG)
    col = lax.broadcasted_iota(jnp.int32, (1, cols), 1)

    steps = req_dev // REQ_STEP
    lse = jnp.zeros((heads, hd), jnp.float32)

    def scores(t):
        for i in range(REQ_STEP):
            r = t * REQ_STEP + i
            q = bf16(q_scr[r * heads : (r + 1) * heads, :])
            s_scr[t % 2, i] = lax.dot_general(q, kv_ref[r, :, 0:hd], NT, preferred_element_type=jnp.float32)

    def weights(t, lse):
        for i in range(REQ_STEP):
            r = t * REQ_STEP + i
            past = jnp.where(col < len_ref[r] * kv_heads, 0.0, NEG)
            s = s_scr[t % 2, i] * scale + (bias_scr[...] + past)
            top = jnp.max(s, axis=1, keepdims=True)
            w = jnp.exp2(s - top)
            total = jnp.sum(w, axis=1, keepdims=True)
            w_scr[t % 2, i] = bf16(w)
            t_scr[t % 2, i] = jnp.broadcast_to(total, (heads, hd))
            lse = jnp.where((lane % req_dev) == r, top * LN2 + jnp.log(total), lse)
        return lse

    def mix(t):
        for i in range(REQ_STEP):
            r = t * REQ_STEP + i
            o = jnp.dot(w_scr[t % 2, i], kv_ref[r, :, hd:], preferred_element_type=jnp.float32)
            o_scr[pl.ds(r, heads, stride=stride), :] = o / t_scr[t % 2, i]

    for t in range(steps + 2):
        if t < steps:
            fetch(t).wait()
            scores(t)
        if 0 <= t - 1 < steps:
            lse = weights(t - 1, lse)
        if t >= 2:
            mix(t - 2)

    hi = f32(bf16(lse))
    rest = lse - hi
    mid = f32(bf16(rest))
    low = rest - mid
    extra = jnp.where(lane < req_dev, hi, jnp.where(lane < 2 * req_dev, mid, low))
    extra = jnp.where(lane < 3 * req_dev, extra, owner_ref[...])
    o_scr[pl.ds(req_dev, heads, stride=stride), :] = extra
    o_scr[pl.ds(req_dev + 1, heads, stride=stride), :] = jnp.zeros((heads, hd), jnp.float32)
    n = out_ref.shape[0]
    c = n // 17 if n % 17 == 0 else n

    @pl.loop(0, n // c)
    def _(k):
        at = pl.ds(pl.multiple_of(k * c, 16), c)
        out_ref[at, :] = bf16(o_scr[at, :])


def suffix_attention(got, owner_row, cache, suffix_len, kv_heads):
    req_dev, cols, width = cache.shape
    hd = width // 2
    heads = got.shape[0]
    rows = heads * (req_dev + 2)
    kernel = functools.partial(suffix_kernel, req_dev=req_dev, heads=heads, kv_heads=kv_heads)
    vmem = pl.BlockSpec(memory_space=pltpu.VMEM)
    return pl.pallas_call(
        kernel,
        name="suffix",
        out_shape=jax.ShapeDtypeStruct((rows, hd), jnp.bfloat16),
        in_specs=[pl.BlockSpec(memory_space=pltpu.SMEM), vmem, vmem, pl.BlockSpec(memory_space=pltpu.HBM)],
        out_specs=vmem,
        scratch_shapes=[
            pltpu.VMEM(cache.shape, cache.dtype),
            pltpu.SemaphoreType.DMA((req_dev // REQ_STEP,)),
            pltpu.VMEM((req_dev * heads, hd), jnp.float32),
            pltpu.VMEM((rows, hd), jnp.float32),
            pltpu.VMEM((2, REQ_STEP, heads, cols), jnp.float32),
            pltpu.VMEM((2, REQ_STEP, heads, cols), jnp.bfloat16),
            pltpu.VMEM((2, REQ_STEP, heads, hd), jnp.float32),
            pltpu.VMEM((heads, cols), jnp.float32),
        ],
        compiler_params=pltpu.CompilerParams(vmem_limit_bytes=57 << 20),
        cost_estimate=pl.CostEstimate(
            flops=4 * req_dev * heads * cols * hd,
            bytes_accessed=2 * cache.size,
            transcendentals=req_dev * heads * cols,
        ),
    )(suffix_len, got, owner_row, cache)


def prefix_kernel(count_ref, q_ref, *refs, req_dev, n_chunks, block, last):
    chunks, refs = refs[:n_chunks], refs[n_chunks:]
    if last:
        prev_o_ref, prev_lse_ref = refs[:2]
        refs = refs[2:]
    o_ref, lse_ref, k_scr, v_scr, s_scr, top_scr, sum_scr, acc_scr = refs
    n_prefix = o_ref.shape[0]
    hd = q_ref.shape[1]
    pages, both = chunks[0].shape[:2]
    tok = both // 2
    page = tok * n_chunks
    scale = hd**-0.5 * LOG2E
    tail = k_scr.shape[0] - pages * page
    row_block = top_scr.shape[0]
    groups = row_block // req_dev

    @pl.loop(0, pages)
    def _(p):
        for c in range(0, n_chunks, 2):
            a, b = f32(chunks[c][p]), f32(chunks[c + 1][p])
            at = pl.ds(pl.multiple_of(p * page + c * tok, 2 * tok), 2 * tok)
            k_scr[at, :] = bf16(jnp.concatenate([a[:tok], b[:tok]], axis=0))
            v_scr[at, :] = bf16(jnp.concatenate([a[tok:], b[tok:]], axis=0))

    k_scr[pl.ds(pages * page, tail), :] = jnp.zeros((tail, hd), jnp.bfloat16)
    v_scr[pl.ds(pages * page, tail), :] = jnp.zeros((tail, hd), jnp.bfloat16)

    col = lax.broadcasted_iota(jnp.int32, (1, block), 1)
    tiles = [slice(k, k + hd) for k in range(0, block, hd)]
    if last:
        lane = lax.broadcasted_iota(jnp.int32, (req_dev, lse_ref.shape[2]), 1)
        lse_ref[...] = jnp.zeros_like(lse_ref)

    def one_prefix(p, first):
        start = first * page
        live = count_ref[p] * page
        steps = (live + block - 1) // block

        @pl.loop(0, q_ref.shape[0] // row_block)
        def _(rb):
            rows = pl.ds(pl.multiple_of(rb * row_block, row_block), row_block)
            top_scr[...] = jnp.full_like(top_scr, NEG)

            @pl.loop(0, steps)
            def _(b):
                at = pl.ds(pl.multiple_of(start + b * block, page), block)
                s = lax.dot_general(q_ref[rows, :], k_scr[at, :], NT, preferred_element_type=jnp.float32)
                s = s + jnp.where(col < live - b * block, 0.0, NEG)
                s_scr[b] = s
                top_scr[...] = jnp.maximum(top_scr[...], functools.reduce(jnp.maximum, [s[:, k] for k in tiles]))

            top = jnp.max(top_scr[...], axis=1, keepdims=True) * scale
            top = jnp.broadcast_to(top, top_scr.shape)
            if last:
                prev = prev_lse_ref[p, rows, :] * LOG2E
                top = jnp.maximum(top, prev)
                acc_scr[...] = f32(prev_o_ref[p, rows, :]) * jnp.exp2(prev - top)
            else:
                acc_scr[...] = jnp.zeros_like(acc_scr)
            top_scr[...] = top
            sum_scr[...] = jnp.zeros_like(sum_scr)

            @pl.loop(0, steps)
            def _(b):
                at = pl.ds(pl.multiple_of(start + b * block, page), block)
                parts = [jnp.exp2(s_scr[b, :, k] * scale - top_scr[...]) for k in tiles]
                sum_scr[...] += functools.reduce(jnp.add, parts)
                w = jnp.concatenate([bf16(x) for x in parts], axis=1)
                acc_scr[...] += jnp.dot(w, v_scr[at, :], preferred_element_type=jnp.float32)

            total = jnp.broadcast_to(jnp.sum(sum_scr[...], axis=1, keepdims=True), sum_scr.shape)
            if last:
                total = total + jnp.exp2(prev_lse_ref[p, rows, :] * LOG2E - top_scr[...])
            o_ref[p, rows, :] = bf16(acc_scr[...] / total)
            value = top_scr[...] * LN2 + jnp.log(total)
            if last:
                lse = lse_ref[p]
                for k in range(groups):
                    lse = jnp.where(lane == rb * groups + k, value[k * req_dev : (k + 1) * req_dev, :], lse)
                lse_ref[p] = lse
            else:
                lse_ref[p, rows, :] = value

        return first + count_ref[p]

    lax.fori_loop(0, n_prefix, one_prefix, 0)


def prefix_attention(queries, chunks, page_counts, req_dev, block, earlier=()):
    n_rows, hd = queries.shape
    n_prefix = page_counts.shape[0]
    pages, both, _ = chunks[0].shape
    tokens = pages * (both // 2) * len(chunks)
    last = len(earlier) > 0
    row_block = min(ROW_BLOCK, n_rows)
    vmem = pl.BlockSpec(memory_space=pltpu.VMEM)
    kernel = functools.partial(prefix_kernel, req_dev=req_dev, n_chunks=len(chunks), block=block, last=last)
    return pl.pallas_call(
        kernel,
        name="prefix" if last else "prefix_early",
        out_shape=(
            jax.ShapeDtypeStruct((n_prefix, n_rows, hd), jnp.bfloat16),
            jax.ShapeDtypeStruct((n_prefix, req_dev if last else n_rows, hd), jnp.float32),
        ),
        in_specs=[pl.BlockSpec(memory_space=pltpu.SMEM)] + [vmem] * (1 + len(chunks) + len(earlier)),
        out_specs=(vmem, vmem),
        scratch_shapes=[
            pltpu.VMEM((tokens + block, hd), jnp.bfloat16),
            pltpu.VMEM((tokens + block, hd), jnp.bfloat16),
            pltpu.VMEM((pl.cdiv(tokens // 2, block), row_block, block), jnp.float32),
            pltpu.VMEM((row_block, hd), jnp.float32),
            pltpu.VMEM((row_block, hd), jnp.float32),
            pltpu.VMEM((row_block, hd), jnp.float32),
        ],
        compiler_params=pltpu.CompilerParams(vmem_limit_bytes=(40 << 20) if last else (24 << 20)),
        cost_estimate=pl.CostEstimate(
            flops=4 * n_rows * tokens * hd, bytes_accessed=4 * n_rows * hd, transcendentals=n_rows * tokens
        ),
    )(page_counts, queries, *chunks, *earlier)


def combine_kernel(got_ref, o_ref, lse_ref, out_ref, scr, *, req_dev):
    n, hd = scr.shape
    stride = req_dev + 2
    blocks = n // stride
    n_prefix = o_ref.shape[0]
    c = n // 17 if n % 17 == 0 else n

    @pl.loop(0, n // c)
    def _(k):
        at = pl.ds(pl.multiple_of(k * c, 16), c)
        scr[at, :] = f32(got_ref[at, :])

    extra = scr[pl.ds(req_dev, blocks, stride=stride), :].T
    tall = [extra[k * req_dev : (k + 1) * req_dev, :] for k in range(4)]
    suffix_lse = tall[0] + tall[1] + tall[2]
    owner = tall[3]
    prefix_lse = lse_ref[0][:, 0:blocks]
    for p in range(1, n_prefix):
        prefix_lse = jnp.where(owner == p, lse_ref[p][:, 0:blocks], prefix_lse)
    top = jnp.maximum(suffix_lse, prefix_lse)
    ws = jnp.exp(suffix_lse - top)
    wp = jnp.exp(prefix_lse - top)
    inverse = 1.0 / (ws + wp)
    ws, wp = ws * inverse, wp * inverse
    for j in range(blocks):
        rows = slice(j * req_dev, (j + 1) * req_dev)
        own = jnp.broadcast_to(owner[:, j : j + 1], (req_dev, hd))
        part = f32(o_ref[0, rows, :])
        for p in range(1, n_prefix):
            part = jnp.where(own == p, f32(o_ref[p, rows, :]), part)
        mine = scr[pl.ds(j * stride, req_dev), :]
        out_ref[rows, :] = bf16(mine * ws[:, j : j + 1] + part * wp[:, j : j + 1])


def combine(got, prefix_o, prefix_lse, req_dev):
    n_rows, hd = prefix_o.shape[1:]
    vmem = pl.BlockSpec(memory_space=pltpu.VMEM)
    return pl.pallas_call(
        functools.partial(combine_kernel, req_dev=req_dev),
        name="combine",
        out_shape=jax.ShapeDtypeStruct((n_rows, hd), jnp.bfloat16),
        in_specs=[vmem] * 3,
        out_specs=vmem,
        scratch_shapes=[pltpu.VMEM(got.shape, jnp.float32)],
        compiler_params=pltpu.CompilerParams(vmem_limit_bytes=16 << 20),
        cost_estimate=pl.CostEstimate(flops=10 * n_rows * hd, bytes_accessed=12 * n_rows * hd, transcendentals=0),
    )(got, prefix_o, prefix_lse)


def exchange(x):
    return lax.all_to_all(x, BLK, split_axis=0, concat_axis=0, tiled=True)


def body(queries, prefix_kv, page_counts, request_prefix, suffix_kv, suffix_len):
    blocks = lax.axis_size(BLK)
    req_dev = suffix_kv.shape[0]
    kv_heads = suffix_kv.shape[2]
    hd = suffix_kv.shape[3] // 2
    page = prefix_kv.shape[1]
    share = blocks // kv_heads
    tok = page // share

    mine = prefix_kv[0].reshape(share, tok, kv_heads, 2, hd).transpose(2, 0, 3, 1, 4)
    mine = mine.reshape(blocks, 2 * tok, hd)
    got = exchange(jnp.concatenate([queries.reshape(blocks, req_dev, hd), mine], axis=1))

    own = got[:, req_dev:, :]
    chips = lax.axis_size("chip")
    swap = [(i, CORES - 1 - i) for i in range(CORES)]
    owner = request_prefix[:, 0].astype(jnp.float32)[None, :]
    owner_row = jnp.pad(owner, ((0, 0), (hd - req_dev, 0)))
    turned = [
        lax.ppermute(own, "chip", [(i, (i + k) % chips) for i in range(chips)]) for k in range(1, chips)
    ]
    cache = suffix_kv.reshape(req_dev, -1, 2 * hd)
    sent = suffix_attention(got, owner_row, cache, suffix_len, kv_heads)
    back = exchange(sent.reshape(blocks, (req_dev + 2) // 2, 2, hd)).reshape(sent.shape)
    chunks = [own, lax.ppermute(own, "core", swap)]
    earlier = prefix_attention(queries, chunks, page_counts, req_dev, EARLY_BLOCK)
    chunks = turned + [lax.ppermute(c, "core", swap) for c in turned]
    prefix_o, prefix_lse = prefix_attention(queries, chunks, page_counts, req_dev, LATE_BLOCK, earlier)
    return combine(back, prefix_o, prefix_lse, req_dev)


def solution(mesh):
    chips = mesh.shape["blk"] // (SEGS * CORES)
    split = Mesh(
        mesh.devices.reshape(mesh.shape["groups"], SEGS, chips, CORES), ("groups", "seg", "chip", "core")
    )
    in_specs = (
        P("groups", BLK),
        P(GROUPS_BLK, None, None, None),
        P("groups"),
        P(GROUPS_BLK, None),
        P(GROUPS_BLK, None, None, None),
        P(GROUPS_BLK),
    )
    return jax.shard_map(body, mesh=split, in_specs=in_specs, out_specs=P("groups", BLK), check_vma=False)
```

```python
import functools

import jax
import jax.numpy as jnp
from jax import lax
from jax.experimental import pallas as pl
from jax.experimental.pallas import tpu as pltpu
from jax.sharding import Mesh
from jax.sharding import PartitionSpec as P

SEGS = 8
CORES = 2
BLK = ("seg", "chip", "core")
GROUPS_BLK = ("groups", "seg", "chip", "core")


LOG2E = 1.4426950408889634
LN2 = 0.6931471805599453
NEG = -1e30

REQ_STEP = 4
EARLY_BLOCK = 256
LATE_BLOCK = 512
ROW_BLOCK = 2048

NT = (((1,), (1,)), ((), ()))


def f32(x):
    return x.astype(jnp.float32)


def bf16(x):
    return x.astype(jnp.bfloat16)


def pack_kernel(q_ref, page_ref, out_ref, page_scr, key_scr, value_scr, sems):
    req_dev = q_ref.shape[1]
    page, kv_heads, width = page_ref.shape
    hd = width // 2
    share = out_ref.shape[0] // kv_heads
    tok = page // share
    fetch = pltpu.make_async_copy(page_ref, page_scr, sems.at[0])
    place = pltpu.make_async_copy(q_ref, out_ref.at[:, pl.ds(0, req_dev), :], sems.at[1])
    fetch.start()
    place.start()
    fetch.wait()
    for t in range(0, page, tok):
        at = slice(t * kv_heads, (t + tok) * kv_heads)
        key_scr[at, :] = f32(page_scr[t : t + tok, :, 0:hd]).reshape(tok * kv_heads, hd)
        value_scr[at, :] = f32(page_scr[t : t + tok, :, hd:width]).reshape(tok * kv_heads, hd)
    for g in range(kv_heads):
        for j in range(share):
            at = pl.ds(j * tok * kv_heads + g, tok, stride=kv_heads)
            keys, values = key_scr[at, :], value_scr[at, :]
            out_ref[g * share + j, req_dev : req_dev + 2 * tok, :] = bf16(jnp.concatenate([keys, values], axis=0))
    place.wait()


def pack(queries, page_kv, blocks):
    n_rows, hd = queries.shape
    page, kv_heads, _ = page_kv.shape
    req_dev = n_rows // blocks
    rows = req_dev + 2 * page * kv_heads // blocks
    return pl.pallas_call(
        pack_kernel,
        name="pack",
        out_shape=jax.ShapeDtypeStruct((blocks, rows, hd), jnp.bfloat16),
        in_specs=[pl.BlockSpec(memory_space=pl.ANY)] * 2,
        out_specs=pl.BlockSpec(memory_space=pltpu.VMEM),
        scratch_shapes=[
            pltpu.VMEM(page_kv.shape, page_kv.dtype),
            pltpu.VMEM((page * kv_heads, hd), jnp.float32),
            pltpu.VMEM((page * kv_heads, hd), jnp.float32),
            pltpu.SemaphoreType.DMA((2,)),
        ],
        compiler_params=pltpu.CompilerParams(vmem_limit_bytes=57 << 20),
        cost_estimate=pl.CostEstimate(flops=0, bytes_accessed=4 * blocks * rows * hd, transcendentals=0),
    )(queries.reshape(blocks, req_dev, hd), page_kv)


def suffix_kernel(
    len_ref, got_ref, owner_ref, cache_ref, out_ref, kv_ref, sems, q_scr, o_scr, s_scr, w_scr, t_scr, bias_scr, *, req_dev, heads, kv_heads
):
    def fetch(step):
        at = pl.ds(step * REQ_STEP, REQ_STEP)
        return pltpu.make_async_copy(cache_ref.at[at], kv_ref.at[at], sems.at[step])

    for step in range(req_dev // REQ_STEP):
        fetch(step).start()
    hd = q_scr.shape[1]
    cols = kv_ref.shape[1]
    stride = out_ref.shape[0] // heads
    scale = hd**-0.5 * LOG2E
    lane = lax.broadcasted_iota(jnp.int32, (heads, hd), 1)

    for h in range(heads):
        q_scr[pl.ds(h, req_dev, stride=heads), :] = f32(got_ref[h, 0:req_dev, :])
    row = lax.broadcasted_iota(jnp.int32, (heads, cols), 0)
    col = lax.broadcasted_iota(jnp.int32, (heads, cols), 1)
    same = (col % kv_heads) == (row // (heads // kv_heads))
    bias_scr[...] = jnp.where(same, 0.0, NEG)
    col = lax.broadcasted_iota(jnp.int32, (1, cols), 1)

    steps = req_dev // REQ_STEP
    lse = jnp.zeros((heads, hd), jnp.float32)

    def scores(t):
        for i in range(REQ_STEP):
            r = t * REQ_STEP + i
            q = bf16(q_scr[r * heads : (r + 1) * heads, :])
            s_scr[t % 2, i] = lax.dot_general(q, kv_ref[r, :, 0:hd], NT, preferred_element_type=jnp.float32)

    def weights(t, lse):
        for i in range(REQ_STEP):
            r = t * REQ_STEP + i
            past = jnp.where(col < len_ref[r] * kv_heads, 0.0, NEG)
            s = s_scr[t % 2, i] * scale + (bias_scr[...] + past)
            top = jnp.max(s, axis=1, keepdims=True)
            w = jnp.exp2(s - top)
            total = jnp.sum(w, axis=1, keepdims=True)
            w_scr[t % 2, i] = bf16(w)
            t_scr[t % 2, i] = jnp.broadcast_to(total, (heads, hd))
            lse = jnp.where((lane % req_dev) == r, top * LN2 + jnp.log(total), lse)
        return lse

    def mix(t):
        for i in range(REQ_STEP):
            r = t * REQ_STEP + i
            o = jnp.dot(w_scr[t % 2, i], kv_ref[r, :, hd:], preferred_element_type=jnp.float32)
            o_scr[pl.ds(r, heads, stride=stride), :] = o / t_scr[t % 2, i]

    for t in range(steps + 2):
        if t < steps:
            fetch(t).wait()
            scores(t)
        if 0 <= t - 1 < steps:
            lse = weights(t - 1, lse)
        if t >= 2:
            mix(t - 2)

    hi = f32(bf16(lse))
    rest = lse - hi
    mid = f32(bf16(rest))
    low = rest - mid
    extra = jnp.where(lane < req_dev, hi, jnp.where(lane < 2 * req_dev, mid, low))
    extra = jnp.where(lane < 3 * req_dev, extra, owner_ref[...])
    o_scr[pl.ds(req_dev, heads, stride=stride), :] = extra
    o_scr[pl.ds(req_dev + 1, heads, stride=stride), :] = jnp.zeros((heads, hd), jnp.float32)
    n = out_ref.shape[0]
    c = n // 17 if n % 17 == 0 else n

    @pl.loop(0, n // c)
    def _(k):
        at = pl.ds(pl.multiple_of(k * c, 16), c)
        out_ref[at, :] = bf16(o_scr[at, :])


def suffix_attention(got, owner_row, cache, suffix_len, kv_heads):
    req_dev, cols, width = cache.shape
    hd = width // 2
    heads = got.shape[0]
    rows = heads * (req_dev + 2)
    kernel = functools.partial(suffix_kernel, req_dev=req_dev, heads=heads, kv_heads=kv_heads)
    vmem = pl.BlockSpec(memory_space=pltpu.VMEM)
    return pl.pallas_call(
        kernel,
        name="suffix",
        out_shape=jax.ShapeDtypeStruct((rows, hd), jnp.bfloat16),
        in_specs=[pl.BlockSpec(memory_space=pltpu.SMEM), vmem, vmem, pl.BlockSpec(memory_space=pltpu.HBM)],
        out_specs=vmem,
        scratch_shapes=[
            pltpu.VMEM(cache.shape, cache.dtype),
            pltpu.SemaphoreType.DMA((req_dev // REQ_STEP,)),
            pltpu.VMEM((req_dev * heads, hd), jnp.float32),
            pltpu.VMEM((rows, hd), jnp.float32),
            pltpu.VMEM((2, REQ_STEP, heads, cols), jnp.float32),
            pltpu.VMEM((2, REQ_STEP, heads, cols), jnp.bfloat16),
            pltpu.VMEM((2, REQ_STEP, heads, hd), jnp.float32),
            pltpu.VMEM((heads, cols), jnp.float32),
        ],
        compiler_params=pltpu.CompilerParams(vmem_limit_bytes=57 << 20),
        cost_estimate=pl.CostEstimate(
            flops=4 * req_dev * heads * cols * hd,
            bytes_accessed=2 * cache.size,
            transcendentals=req_dev * heads * cols,
        ),
    )(suffix_len, got, owner_row, cache)


def prefix_kernel(count_ref, q_ref, *refs, req_dev, n_chunks, block, last):
    chunks, refs = refs[:n_chunks], refs[n_chunks:]
    if last:
        prev_o_ref, prev_lse_ref = refs[:2]
        refs = refs[2:]
    o_ref, lse_ref, k_scr, v_scr, s_scr, top_scr, sum_scr, acc_scr = refs
    n_prefix = o_ref.shape[0]
    hd = q_ref.shape[1]
    pages, both = chunks[0].shape[:2]
    tok = both // 2
    page = tok * n_chunks
    scale = hd**-0.5 * LOG2E
    tail = k_scr.shape[0] - pages * page
    row_block = top_scr.shape[0]
    groups = row_block // req_dev

    @pl.loop(0, pages)
    def _(p):
        for c in range(0, n_chunks, 2):
            a, b = f32(chunks[c][p]), f32(chunks[c + 1][p])
            at = pl.ds(pl.multiple_of(p * page + c * tok, 2 * tok), 2 * tok)
            k_scr[at, :] = bf16(jnp.concatenate([a[:tok], b[:tok]], axis=0))
            v_scr[at, :] = bf16(jnp.concatenate([a[tok:], b[tok:]], axis=0))

    k_scr[pl.ds(pages * page, tail), :] = jnp.zeros((tail, hd), jnp.bfloat16)
    v_scr[pl.ds(pages * page, tail), :] = jnp.zeros((tail, hd), jnp.bfloat16)

    col = lax.broadcasted_iota(jnp.int32, (1, block), 1)
    tiles = [slice(k, k + hd) for k in range(0, block, hd)]
    if last:
        lane = lax.broadcasted_iota(jnp.int32, (req_dev, lse_ref.shape[2]), 1)
        lse_ref[...] = jnp.zeros_like(lse_ref)

    def one_prefix(p, first):
        start = first * page
        live = count_ref[p] * page
        steps = (live + block - 1) // block

        @pl.loop(0, q_ref.shape[0] // row_block)
        def _(rb):
            rows = pl.ds(pl.multiple_of(rb * row_block, row_block), row_block)
            top_scr[...] = jnp.full_like(top_scr, NEG)

            @pl.loop(0, steps)
            def _(b):
                at = pl.ds(pl.multiple_of(start + b * block, page), block)
                s = lax.dot_general(q_ref[rows, :], k_scr[at, :], NT, preferred_element_type=jnp.float32)
                s = s + jnp.where(col < live - b * block, 0.0, NEG)
                s_scr[b] = s
                top_scr[...] = jnp.maximum(top_scr[...], functools.reduce(jnp.maximum, [s[:, k] for k in tiles]))

            top = jnp.max(top_scr[...], axis=1, keepdims=True) * scale
            top = jnp.broadcast_to(top, top_scr.shape)
            if last:
                prev = prev_lse_ref[p, rows, :] * LOG2E
                top = jnp.maximum(top, prev)
                acc_scr[...] = f32(prev_o_ref[p, rows, :]) * jnp.exp2(prev - top)
            else:
                acc_scr[...] = jnp.zeros_like(acc_scr)
            top_scr[...] = top
            sum_scr[...] = jnp.zeros_like(sum_scr)

            @pl.loop(0, steps)
            def _(b):
                at = pl.ds(pl.multiple_of(start + b * block, page), block)
                parts = [jnp.exp2(s_scr[b, :, k] * scale - top_scr[...]) for k in tiles]
                sum_scr[...] += functools.reduce(jnp.add, parts)
                w = jnp.concatenate([bf16(x) for x in parts], axis=1)
                acc_scr[...] += jnp.dot(w, v_scr[at, :], preferred_element_type=jnp.float32)

            total = jnp.broadcast_to(jnp.sum(sum_scr[...], axis=1, keepdims=True), sum_scr.shape)
            if last:
                total = total + jnp.exp2(prev_lse_ref[p, rows, :] * LOG2E - top_scr[...])
            o_ref[p, rows, :] = bf16(acc_scr[...] / total)
            value = top_scr[...] * LN2 + jnp.log(total)
            if last:
                lse = lse_ref[p]
                for k in range(groups):
                    lse = jnp.where(lane == rb * groups + k, value[k * req_dev : (k + 1) * req_dev, :], lse)
                lse_ref[p] = lse
            else:
                lse_ref[p, rows, :] = value

        return first + count_ref[p]

    lax.fori_loop(0, n_prefix, one_prefix, 0)


def prefix_attention(queries, chunks, page_counts, req_dev, block, earlier=()):
    n_rows, hd = queries.shape
    n_prefix = page_counts.shape[0]
    pages, both, _ = chunks[0].shape
    tokens = pages * (both // 2) * len(chunks)
    last = len(earlier) > 0
    row_block = min(ROW_BLOCK, n_rows)
    vmem = pl.BlockSpec(memory_space=pltpu.VMEM)
    kernel = functools.partial(prefix_kernel, req_dev=req_dev, n_chunks=len(chunks), block=block, last=last)
    return pl.pallas_call(
        kernel,
        name="prefix" if last else "prefix_early",
        out_shape=(
            jax.ShapeDtypeStruct((n_prefix, n_rows, hd), jnp.bfloat16),
            jax.ShapeDtypeStruct((n_prefix, req_dev if last else n_rows, hd), jnp.float32),
        ),
        in_specs=[pl.BlockSpec(memory_space=pltpu.SMEM)] + [vmem] * (1 + len(chunks) + len(earlier)),
        out_specs=(vmem, vmem),
        scratch_shapes=[
            pltpu.VMEM((tokens + block, hd), jnp.bfloat16),
            pltpu.VMEM((tokens + block, hd), jnp.bfloat16),
            pltpu.VMEM((pl.cdiv(tokens // 2, block), row_block, block), jnp.float32),
            pltpu.VMEM((row_block, hd), jnp.float32),
            pltpu.VMEM((row_block, hd), jnp.float32),
            pltpu.VMEM((row_block, hd), jnp.float32),
        ],
        compiler_params=pltpu.CompilerParams(vmem_limit_bytes=(40 << 20) if last else (24 << 20)),
        cost_estimate=pl.CostEstimate(
            flops=4 * n_rows * tokens * hd, bytes_accessed=4 * n_rows * hd, transcendentals=n_rows * tokens
        ),
    )(page_counts, queries, *chunks, *earlier)


def combine_kernel(got_ref, o_ref, lse_ref, out_ref, scr, *, req_dev):
    n, hd = scr.shape
    stride = req_dev + 2
    blocks = n // stride
    n_prefix = o_ref.shape[0]
    c = n // 17 if n % 17 == 0 else n

    @pl.loop(0, n // c)
    def _(k):
        at = pl.ds(pl.multiple_of(k * c, 16), c)
        scr[at, :] = f32(got_ref[at, :])

    extra = scr[pl.ds(req_dev, blocks, stride=stride), :].T
    tall = [extra[k * req_dev : (k + 1) * req_dev, :] for k in range(4)]
    suffix_lse = tall[0] + tall[1] + tall[2]
    owner = tall[3]
    prefix_lse = lse_ref[0][:, 0:blocks]
    for p in range(1, n_prefix):
        prefix_lse = jnp.where(owner == p, lse_ref[p][:, 0:blocks], prefix_lse)
    top = jnp.maximum(suffix_lse, prefix_lse)
    ws = jnp.exp(suffix_lse - top)
    wp = jnp.exp(prefix_lse - top)
    inverse = 1.0 / (ws + wp)
    ws, wp = ws * inverse, wp * inverse
    for j in range(blocks):
        rows = slice(j * req_dev, (j + 1) * req_dev)
        own = jnp.broadcast_to(owner[:, j : j + 1], (req_dev, hd))
        part = f32(o_ref[0, rows, :])
        for p in range(1, n_prefix):
            part = jnp.where(own == p, f32(o_ref[p, rows, :]), part)
        mine = scr[pl.ds(j * stride, req_dev), :]
        out_ref[rows, :] = bf16(mine * ws[:, j : j + 1] + part * wp[:, j : j + 1])


def combine(got, prefix_o, prefix_lse, req_dev):
    n_rows, hd = prefix_o.shape[1:]
    vmem = pl.BlockSpec(memory_space=pltpu.VMEM)
    return pl.pallas_call(
        functools.partial(combine_kernel, req_dev=req_dev),
        name="combine",
        out_shape=jax.ShapeDtypeStruct((n_rows, hd), jnp.bfloat16),
        in_specs=[vmem] * 3,
        out_specs=vmem,
        scratch_shapes=[pltpu.VMEM(got.shape, jnp.float32)],
        compiler_params=pltpu.CompilerParams(vmem_limit_bytes=16 << 20),
        cost_estimate=pl.CostEstimate(flops=10 * n_rows * hd, bytes_accessed=12 * n_rows * hd, transcendentals=0),
    )(got, prefix_o, prefix_lse)


def exchange(x):
    return lax.all_to_all(x, BLK, split_axis=0, concat_axis=0, tiled=True)


def body(queries, prefix_kv, page_counts, request_prefix, suffix_kv, suffix_len):
    blocks = lax.axis_size(BLK)
    req_dev = suffix_kv.shape[0]
    kv_heads = suffix_kv.shape[2]
    hd = suffix_kv.shape[3] // 2
    got = exchange(pack(queries, prefix_kv[0], blocks))

    own = got[:, req_dev:, :]
    chips = lax.axis_size("chip")
    swap = [(i, CORES - 1 - i) for i in range(CORES)]
    owner = request_prefix[:, 0].astype(jnp.float32)[None, :]
    owner_row = jnp.pad(owner, ((0, 0), (hd - req_dev, 0)))
    turned = [
        lax.ppermute(own, "chip", [(i, (i + k) % chips) for i in range(chips)]) for k in range(1, chips)
    ]
    cache = suffix_kv.reshape(req_dev, -1, 2 * hd)
    sent = suffix_attention(got, owner_row, cache, suffix_len, kv_heads)
    back = exchange(sent.reshape(blocks, (req_dev + 2) // 2, 2, hd)).reshape(sent.shape)
    chunks = [own, lax.ppermute(own, "core", swap)]
    earlier = prefix_attention(queries, chunks, page_counts, req_dev, EARLY_BLOCK)
    chunks = turned + [lax.ppermute(c, "core", swap) for c in turned]
    prefix_o, prefix_lse = prefix_attention(queries, chunks, page_counts, req_dev, LATE_BLOCK, earlier)
    return combine(back, prefix_o, prefix_lse, req_dev)


def solution(mesh):
    chips = mesh.shape["blk"] // (SEGS * CORES)
    split = Mesh(
        mesh.devices.reshape(mesh.shape["groups"], SEGS, chips, CORES), ("groups", "seg", "chip", "core")
    )
    in_specs = (
        P("groups", BLK),
        P(GROUPS_BLK, None, None, None),
        P("groups"),
        P(GROUPS_BLK, None),
        P(GROUPS_BLK, None, None, None),
        P(GROUPS_BLK),
    )
    return jax.shard_map(body, mesh=split, in_specs=in_specs, out_specs=P("groups", BLK), check_vma=False)
```
